32 devices in a mesh: first: 8 (over z, core), second: 4 (over y, x).
Axes of the slice: x: 2, y: 2, z: 4, core: 2. Of those that a mesh axis runs over, the one named last changes fastest.
Arguments:
- pair_rows: bfloat16 [96, 96, 128], P('first', 'second'), may hold values from -6 to 6
- in_gain: float32 [128], replicated, may hold values from 0.25 to 1.75
- left_weight: bfloat16 [128, 128], replicated, may hold values from -0.5 to 0.5
- right_weight: bfloat16 [128, 128], replicated, may hold values from -0.5 to 0.5
- mid_gain: float32 [128], replicated, may hold values from 0.25 to 1.75
- out_weight: bfloat16 [128, 128], replicated, may hold values from -0.5 to 0.5
- out_gate: bfloat16 [128, 128], replicated, may hold values from -0.5 to 0.5
Outputs:
- triangle_out: bfloat16 [96, 96, 128], P('first', 'second')
The draws below stay inside these ranges and needn't reach their ends.
All inputs are finite; a program needn't handle non-finite values.
Results may differ from the reference program's by a relative error of at most 0.012.
Values may be sent and summed in bfloat16 or wider, within the bound.
No kernel may reach another device: no remote copies, remote signals or barrier semaphores. Data moves between devices by JAX's collectives and lax.ppermute only.
A program may use at most 64 MiB of HBM per device.

```python
import jax
import jax.numpy as jnp
from jax import lax

RESIDUES = 96
PAIR_WIDTH = 128
MIX_WIDTH = 128


def steps_of(stream_key, dims, cuts, smallest, top_value):
    def one(position, shards_of):
        draws = jax.random.uniform(jax.random.fold_in(jax.random.fold_in(stream_key, 6), position), (shards_of,), jnp.float32, smallest / len(cuts), top_value / len(cuts))
        return jnp.repeat(jnp.exp(draws), dims[position] // shards_of).reshape((-1,) + (1,) * (len(dims) - position - 1))

    level = one(*cuts[0])
    for cut in cuts[1:]:
        level = level * one(*cut)
    return level


def gaussian(stream_key, dims, spread, limit, cuts=(), held_as=jnp.bfloat16):
    values = spread * jax.random.normal(stream_key, dims, jnp.float32)
    if cuts:
        values = values * steps_of(stream_key, dims, cuts, -0.22, 0.18)
    return jnp.clip(values, -limit, limit).astype(held_as)


def setup_inputs(seed: int = 0) -> dict:
    key_list = jax.random.split(jax.random.key(seed), 8)
    pair_rows = gaussian(key_list[0], (RESIDUES, RESIDUES, PAIR_WIDTH), 1.0, 6.0, ((0, 8), (1, 4)))
    in_gain = jnp.clip(1.0 + 0.15 * jax.random.normal(key_list[1], (PAIR_WIDTH,), jnp.float32), 0.25, 1.75)
    left_weight = gaussian(key_list[2], (PAIR_WIDTH, MIX_WIDTH), PAIR_WIDTH ** -0.5, 0.5)
    right_weight = gaussian(key_list[3], (PAIR_WIDTH, MIX_WIDTH), PAIR_WIDTH ** -0.5, 0.5)
    mid_gain = jnp.clip(1.0 + 0.15 * jax.random.normal(key_list[4], (MIX_WIDTH,), jnp.float32), 0.25, 1.75)
    out_weight = gaussian(key_list[5], (MIX_WIDTH, PAIR_WIDTH), MIX_WIDTH ** -0.5, 0.5)
    out_gate = gaussian(key_list[6], (PAIR_WIDTH, PAIR_WIDTH), PAIR_WIDTH ** -0.5, 0.5)
    return {"pair_rows": pair_rows, "in_gain": in_gain, "left_weight": left_weight, "right_weight": right_weight, "mid_gain": mid_gain, "out_weight": out_weight, "out_gate": out_gate}


def norm_channels(values, channel_gain):
    centred = values - lax.optimization_barrier(jnp.mean(values, axis=-1, keepdims=True))
    return centred * lax.rsqrt(lax.optimization_barrier(jnp.mean(centred * centred, axis=-1, keepdims=True)) + 1e-05) * channel_gain

def project_pair(pair_in, in_gain, left_weight, right_weight):
    ready = norm_channels(pair_in.astype(jnp.float32), in_gain).astype(jnp.bfloat16)
    ready = lax.optimization_barrier(ready)
    left = jnp.einsum('ijc,cd->ijd', ready.astype(jnp.float32), left_weight.astype(jnp.float32))
    right = jnp.einsum('ijc,cd->ijd', ready.astype(jnp.float32), right_weight.astype(jnp.float32))
    return (ready, left.astype(jnp.bfloat16), right.astype(jnp.bfloat16))

def to_pair(mixed, ready, mid_gain, out_weight, out_gate):
    scaled = norm_channels(mixed.astype(jnp.float32), mid_gain).astype(jnp.bfloat16)
    scaled = lax.optimization_barrier(scaled)
    gate = jax.nn.sigmoid(jnp.einsum('ijc,cd->ijd', ready.astype(jnp.float32), out_gate.astype(jnp.float32)))
    return (jnp.einsum('ijd,dc->ijc', scaled.astype(jnp.float32), out_weight.astype(jnp.float32)) * gate).astype(jnp.bfloat16)

def reference(pair_rows, in_gain, left_weight, right_weight, mid_gain, out_weight, out_gate):
    ready, left, right = project_pair(pair_rows, in_gain, left_weight, right_weight)
    left, right = lax.optimization_barrier((left, right))

    def one_channel(pair_of):
        return (jnp.dot(pair_of[0].T, pair_of[1], preferred_element_type=jnp.float32) * RESIDUES ** (-0.5)).astype(jnp.bfloat16)
    mixed = jnp.moveaxis(lax.map(one_channel, (jnp.moveaxis(left, -1, 0), jnp.moveaxis(right, -1, 0))), 0, -1)
    mixed = lax.optimization_barrier(mixed)
    return to_pair(mixed, ready, mid_gain, out_weight, out_gate)
```

```python
import functools

import jax
import jax.numpy as jnp
from jax import lax
from jax.experimental import pallas as pl
from jax.experimental.pallas import tpu as pltpu
from jax.sharding import PartitionSpec as P

VMEM = pl.BlockSpec(memory_space=pltpu.VMEM)


def norm_channels(values, channel_gain):
    centred = values - jnp.mean(values, axis=-1, keepdims=True)
    variance = jnp.mean(centred * centred, axis=-1, keepdims=True)
    return centred * lax.rsqrt(variance + 1e-05) * channel_gain


def dot(rows, weight):
    return jnp.dot(rows, weight, preferred_element_type=jnp.float32)


def project(rows, gain, weight):
    ready = norm_channels(rows.astype(jnp.float32), gain).astype(jnp.bfloat16)
    return dot(ready, weight).astype(jnp.bfloat16).astype(jnp.float32)


def core_of():
    return lax.rem(lax.axis_index("first"), 2)


def pack_kernel(mine, other, out, wide):
    rows, columns, _ = mine.shape
    half = columns // 2
    core = core_of()
    for part, block in enumerate((mine, other)):
        for k in range(rows):
            row = block[k].astype(jnp.float32)
            wide[pl.ds((part * rows + k) * half, half)] = jnp.where(
                core == 0, row[:half], row[half:]
            )
    out[...] = wide[...].astype(out.dtype)


def right_kernel(mine, other, gain, weight, out):
    rows, columns, width = mine.shape
    for part, block in enumerate((mine, other)):
        flat = block[...].reshape(rows * columns, width)
        out[pl.ds(part * rows, rows)] = project(flat, gain[...], weight[...]).reshape(
            rows, columns, -1
        )


def gate_kernel(mine, gain, weight, out):
    rows, columns, width = mine.shape
    flat = mine[...].reshape(rows * columns, width).astype(jnp.float32)
    ready = norm_channels(flat, gain[...]).astype(jnp.bfloat16)
    out[...] = jax.nn.sigmoid(dot(ready, weight[...])).reshape(rows, columns, -1)


def partial_kernel(blocks, messages, merge, *refs):
    packed, (gain, weight, right), outs, left = (
        refs[:blocks],
        refs[blocks : blocks + 3],
        refs[blocks + 3 : -1],
        refs[-1],
    )
    first, second = lax.axis_index("first"), lax.axis_index("second")
    chip, core = first // 2, lax.rem(first, 2)
    for step, block in enumerate(packed):
        left[second ^ step] = project(block[...], gain[...], weight[...])
    depth, columns, width = right.shape
    half = left.shape[1] // depth
    group = max(g for g in range(1, half + 1) if half % g == 0 and g * columns <= 288)
    for out, (chips, cores) in zip(outs, messages):
        block = (chip ^ chips) if merge == 1 else 2 * (chip ^ chips) + (core ^ cores)
        for base in range(0, half, group):

            def step(k, sums):
                line = right[k]
                return tuple(
                    total + left[block, pl.ds(k * half + base + i, 1)] * line
                    for i, total in enumerate(sums)
                )

            zero = jnp.zeros((columns, width), jnp.float32)
            sums = lax.fori_loop(0, depth, step, (zero,) * group, unroll=8)
            for i, total in enumerate(sums):
                out[base + i] = total.astype(out.dtype)


def final_kernel(merge, per, scale, *refs):
    parts, (gate, gain, weight, out) = refs[:-4], refs[-4:]
    core = core_of()
    half, columns, width = parts[0].shape
    for slot in range(merge):
        mine = parts[slot * per : (slot + 1) * per]
        total = sum(part[...].astype(jnp.float32) for part in mine)
        flat = total.reshape(half * columns, width) * scale
        scaled = norm_channels(flat, gain[...]).astype(jnp.bfloat16)
        result = dot(scaled, weight[...]).reshape(half, columns, -1)
        rows = pl.ds(0, half) if merge == 1 else pl.ds((core ^ slot) * half, half)
        out[rows] = (result * gate[rows]).astype(out.dtype)


def call(kernel, out_shapes, *operands, scratch=(), flops=0):
    many = isinstance(out_shapes, list)
    return pl.pallas_call(
        kernel,
        out_shape=out_shapes,
        in_specs=[VMEM] * len(operands),
        out_specs=[VMEM] * len(out_shapes) if many else VMEM,
        scratch_shapes=scratch,
        cost_estimate=pl.CostEstimate(flops=flops, bytes_accessed=100000, transcendentals=0),
    )(*operands)


def shards(pair_rows, in_gain, left_weight, right_weight, mid_gain, out_weight, out_gate):
    firsts, seconds = lax.axis_size("first"), lax.axis_size("second")
    rows, columns, width = pair_rows.shape
    mix, wide = left_weight.shape[1], out_weight.shape[1]
    chips, half, depth = firsts // 2, columns // 2, 2 * rows
    merge = rows // half
    in_gain, mid_gain = in_gain.reshape(1, -1), mid_gain.reshape(1, -1)
    axes = ("first", "second")
    shape = jax.ShapeDtypeStruct

    def swap(values, chip=0, core=0, block=0):
        pairs = [
            (a * seconds + b, (a ^ (2 * chip + core)) * seconds + (b ^ block))
            for a in range(firsts)
            for b in range(seconds)
        ]
        return lax.ppermute(values, axes, pairs)

    other = swap(pair_rows, core=1)
    packed = call(
        pack_kernel,
        shape((depth * half, width), pair_rows.dtype),
        pair_rows,
        other,
        scratch=[pltpu.VMEM((depth * half, width), jnp.float32)],
    )
    blocks = [packed] + [swap(packed, block=s) for s in range(1, seconds)]
    right = call(
        right_kernel,
        shape((depth, columns, mix), jnp.float32),
        pair_rows,
        other,
        in_gain,
        right_weight,
        flops=2 * depth * columns * width * mix,
    )
    cores = range(merge)
    order = [2, 3, 1] if chips == 4 else list(range(1, chips))
    messages = [(t, c) for t in order + [0] for c in reversed(cores)]
    sums = call(
        functools.partial(partial_kernel, len(blocks), messages, merge),
        [
            shape((half, columns, mix), jnp.float32 if m == (0, 0) else jnp.bfloat16)
            for m in messages
        ],
        *blocks,
        in_gain,
        left_weight,
        right,
        scratch=[pltpu.VMEM((seconds, depth * half, mix), jnp.float32)],
        flops=2 * seconds * depth * half * width * mix,
    )
    gate = call(
        gate_kernel,
        shape((rows, columns, wide), jnp.float32),
        pair_rows,
        in_gain,
        out_gate,
        flops=2 * rows * columns * width * wide,
    )
    arrived = {
        m: part if m == (0, 0) else swap(part, chip=m[0], core=m[1])
        for m, part in zip(messages, sums)
    }
    parts = [arrived[t, c] for c in cores for t in range(chips)]
    return call(
        functools.partial(final_kernel, merge, chips, (rows * firsts) ** -0.5),
        shape((rows, columns, wide), jnp.bfloat16),
        *parts,
        gate,
        mid_gain,
        out_weight,
        flops=2 * rows * columns * mix * wide,
    )


def solution(mesh):
    in_specs = (P("first", "second", None), P(), P(), P(), P(), P(), P())
    out_specs = P("first", "second", None)
    return jax.shard_map(shards, mesh=mesh, in_specs=in_specs, out_specs=out_specs, check_vma=False)
```

```python
import functools
import math

import jax
import jax.numpy as jnp
from jax import lax
from jax.experimental import pallas as pl
from jax.experimental.pallas import tpu as pltpu
from jax.sharding import PartitionSpec as P

VMEM = pl.BlockSpec(memory_space=pltpu.VMEM)


def norm_channels(values, channel_gain):
    centred = values - jnp.mean(values, axis=-1, keepdims=True)
    variance = jnp.mean(centred * centred, axis=-1, keepdims=True)
    return centred * lax.rsqrt(variance + 1e-05) * channel_gain


def dot(rows, weight):
    return jnp.dot(rows, weight, preferred_element_type=jnp.float32)


def project(rows, gain, weight):
    ready = norm_channels(rows.astype(jnp.float32), gain).astype(jnp.bfloat16)
    return dot(ready, weight).astype(jnp.bfloat16).astype(jnp.float32)


def core_of():
    return lax.rem(lax.axis_index("first"), 2)


def pack_kernel(mine, other, out, wide):
    rows, columns, _ = mine.shape
    half = columns // 2
    core = core_of()
    for part, block in enumerate((mine, other)):
        for k in range(rows):
            row = block[k].astype(jnp.float32)
            wide[pl.ds((part * rows + k) * half, half)] = jnp.where(
                core == 0, row[:half], row[half:]
            )
    out[...] = wide[...].astype(out.dtype)


def own_kernel(*refs):
    count = len(refs) // 2 - 1
    sources, held, (right, gate, done) = refs[:count], refs[count : 2 * count], refs[2 * count :]
    copies = [
        pltpu.make_async_copy(source, target, done.at[i])
        for i, (source, target) in enumerate(zip(sources, held))
    ]
    for copy in copies:
        copy.start()
    for copy in copies:
        copy.wait()
    mine, in_gain, right_weight, gate_weight = held[:4]
    rows, columns, width = mine.shape
    flat = mine[...].reshape(rows * columns, width).astype(jnp.float32)
    ready = norm_channels(flat, in_gain[...]).astype(jnp.bfloat16)
    factor = dot(ready, right_weight[...]).astype(jnp.bfloat16).astype(jnp.float32)
    right[...] = factor.reshape(rows, columns, -1)
    gate[...] = jax.nn.sigmoid(dot(ready, gate_weight[...])).reshape(rows, columns, -1)


def add_block(left, rights, sums, place):
    rows, columns, width = rights[0].shape
    half = left.shape[0] // (2 * rows)
    group = max(g for g in range(1, half + 1) if half % g == 0 and g * columns <= 288)
    for base in range(0, half, group):
        totals = (jnp.zeros((columns, width), jnp.float32),) * group
        for part, right in enumerate(rights):

            def step(k, totals, part=part, right=right):
                line, at = right[k], (part * rows + k) * half + base
                return tuple(
                    total + left[pl.ds(at + i, 1)] * line for i, total in enumerate(totals)
                )

            totals = lax.fori_loop(0, rows, step, totals, unroll=6)
        for i, total in enumerate(totals):
            sums[place, base + i] = total


def first_kernel(packed, other, right, gain, left_weight, right_weight, right_other, sums, left):
    rows, columns, width = other.shape
    flat = other[...].reshape(rows * columns, width)
    right_other[...] = project(flat, gain[...], right_weight[...]).reshape(rows, columns, -1)
    left[...] = project(packed[...], gain[...], left_weight[...])
    add_block(left, (right, right_other), sums, lax.axis_index("second"))


def middle_kernel(steps, *refs):
    (right, right_other, gain, weight, _, sums, left) = refs[len(steps) :]
    for step, block in zip(steps, refs):
        left[...] = project(block[...], gain[...], weight[...])
        add_block(left, (right, right_other), sums, lax.axis_index("second") ^ step)


def last_kernel(step, messages, merge, block, right, right_other, gain, weight, before, *refs):
    *outs, sums, left = refs
    first, second = lax.axis_index("first"), lax.axis_index("second")
    chip, core = first // 2, lax.rem(first, 2)
    left[...] = project(block[...], gain[...], weight[...])
    add_block(left, (right, right_other), sums, second ^ step)
    for out, (chips, cores) in zip(outs, messages):
        place = (chip ^ chips) if merge == 1 else 2 * (chip ^ chips) + (core ^ cores)
        out[...] = sums[place].astype(out.dtype)


def final_kernel(merge, per, scale, *refs):
    parts, (gate, gain, weight, out) = refs[:-4], refs[-4:]
    core = core_of()
    half, columns, width = parts[0].shape
    for slot in range(merge):
        mine = parts[slot * per : (slot + 1) * per]
        total = sum(part[...].astype(jnp.float32) for part in mine)
        flat = total.reshape(half * columns, width) * scale
        scaled = norm_channels(flat, gain[...]).astype(jnp.bfloat16)
        result = dot(scaled, weight[...]).reshape(half, columns, -1)
        rows = pl.ds(0, half) if merge == 1 else pl.ds((core ^ slot) * half, half)
        out[rows] = (result * gate[rows]).astype(out.dtype)


def call(kernel, out_shapes, *operands, scratch=(), waits=(), flops=0, moved=100000, aliases={}, space=pltpu.VMEM):
    many = isinstance(out_shapes, list)
    held = jax.tree.leaves(out_shapes) + list(operands) + list(scratch)
    held = sum(math.prod(ref.shape) * jnp.dtype(ref.dtype).itemsize for ref in held)
    return pl.pallas_call(
        kernel,
        out_shape=out_shapes,
        in_specs=[pl.BlockSpec(memory_space=space)] * len(operands),
        out_specs=[VMEM] * len(out_shapes) if many else VMEM,
        scratch_shapes=[*scratch, *waits],
        input_output_aliases=aliases,
        compiler_params=pltpu.CompilerParams(vmem_limit_bytes=held + (2 << 20)),
        cost_estimate=pl.CostEstimate(flops=flops, bytes_accessed=moved, transcendentals=0),
    )(*operands)


def shards(pair_rows, in_gain, left_weight, right_weight, mid_gain, out_weight, out_gate):
    firsts, seconds = lax.axis_size("first"), lax.axis_size("second")
    rows, columns, width = pair_rows.shape
    mix, wide = left_weight.shape[1], out_weight.shape[1]
    chips, half, depth = firsts // 2, columns // 2, 2 * rows
    merge = rows // half
    in_gain, mid_gain = in_gain.reshape(1, -1), mid_gain.reshape(1, -1)
    axes = ("first", "second")
    shape, f32 = jax.ShapeDtypeStruct, jnp.float32

    def swap(values, chip=0, core=0, block=0):
        pairs = [
            (a * seconds + b, (a ^ (2 * chip + core)) * seconds + (b ^ block))
            for a in range(firsts)
            for b in range(seconds)
        ]
        return lax.ppermute(values, axes, pairs)

    work = 2 * depth * half * width * mix
    lefts = [pltpu.VMEM((depth * half, mix), f32)]
    held = shape((seconds, half, columns, mix), f32)
    other = swap(pair_rows, core=1)
    arguments = (
        pair_rows,
        in_gain,
        right_weight,
        out_gate,
        left_weight,
        mid_gain,
        out_weight,
    )
    mine, in_gain, right_weight, _, left_weight, mid_gain, out_weight, right, gate = call(
        own_kernel,
        [shape(x.shape, x.dtype) for x in arguments]
        + [shape((rows, columns, n), f32) for n in (mix, wide)],
        *[pltpu.with_memory_space_constraint(x, pltpu.HBM) for x in arguments],
        waits=[pltpu.SemaphoreType.DMA((len(arguments),))],
        flops=4 * rows * columns * width * mix,
        moved=0,
        space=pltpu.HBM,
    )
    packed = call(
        pack_kernel,
        shape((depth * half, width), pair_rows.dtype),
        mine,
        other,
        scratch=[pltpu.VMEM((depth * half, width), f32)],
    )
    blocks = [swap(packed, block=s) for s in range(1, seconds)]
    right_other, sums = call(
        first_kernel,
        [shape(right.shape, f32), held],
        packed,
        other,
        right,
        in_gain,
        left_weight,
        right_weight,
        scratch=lefts,
        flops=10 * work,
    )
    factors = (right, right_other, in_gain, left_weight)
    sums = call(
        functools.partial(middle_kernel, list(range(1, seconds - 1))),
        held,
        *blocks[:-1],
        *factors,
        sums,
        scratch=lefts,
        flops=10 * (seconds - 2) * work,
        aliases={seconds + 2: 0},
    )
    cores = range(merge)
    order = [2, 3, 1] if chips == 4 else list(range(1, chips))
    messages = [(t, c) for t in order + [0] for c in reversed(cores)]
    *outgoing, _ = call(
        functools.partial(last_kernel, seconds - 1, messages, merge),
        [shape((half, columns, mix), f32 if m == (0, 0) else jnp.bfloat16) for m in messages]
        + [held],
        blocks[-1],
        *factors,
        sums,
        scratch=lefts,
        flops=10 * work,
        aliases={5: len(messages)},
    )
    arrived = {
        m: part if m == (0, 0) else swap(part, chip=m[0], core=m[1])
        for m, part in zip(messages, outgoing)
    }
    parts = [arrived[t, c] for c in cores for t in range(chips)]
    return call(
        functools.partial(final_kernel, merge, chips, (rows * firsts) ** -0.5),
        shape((rows, columns, wide), jnp.bfloat16),
        *parts,
        gate,
        mid_gain,
        out_weight,
        flops=2 * rows * columns * mix * wide,
    )


def solution(mesh):
    in_specs = (P("first", "second", None), P(), P(), P(), P(), P(), P())
    out_specs = P("first", "second", None)
    return jax.shard_map(shards, mesh=mesh, in_specs=in_specs, out_specs=out_specs, check_vma=False)
```

```python
import functools
import math

import jax
import jax.numpy as jnp
from jax import lax
from jax.experimental import pallas as pl
from jax.experimental.pallas import tpu as pltpu
from jax.sharding import PartitionSpec as P

VMEM = pl.BlockSpec(memory_space=pltpu.VMEM)


def norm_channels(values, channel_gain):
    centred = values - jnp.mean(values, axis=-1, keepdims=True)
    variance = jnp.mean(centred * centred, axis=-1, keepdims=True)
    return centred * lax.rsqrt(variance + 1e-05) * channel_gain


def dot(rows, weight):
    return jnp.dot(rows, weight, preferred_element_type=jnp.float32)


def project(rows, gain, weight):
    ready = norm_channels(rows.astype(jnp.float32), gain).astype(jnp.bfloat16)
    return dot(ready, weight).astype(jnp.bfloat16).astype(jnp.float32)


def core_of():
    return lax.rem(lax.axis_index("first"), 2)


def pack_kernel(mine, other, out, wide):
    rows, columns, _ = mine.shape
    half = columns // 2
    core = core_of()
    for part, block in enumerate((mine, other)):
        for k in range(rows):
            row = block[k].astype(jnp.float32)
            wide[pl.ds((part * rows + k) * half, half)] = jnp.where(
                core == 0, row[:half], row[half:]
            )
    out[...] = wide[...].astype(out.dtype)


def load_kernel(*refs):
    count = len(refs) // 2
    copies = [
        pltpu.make_async_copy(source, target, refs[-1].at[i])
        for i, (source, target) in enumerate(zip(refs[:count], refs[count:-1]))
    ]
    for copy in copies:
        copy.start()
    for copy in copies:
        copy.wait()


def gate_kernel(mine, gain, weight, out):
    rows, columns, width = mine.shape
    flat = mine[...].reshape(rows * columns, width).astype(jnp.float32)
    ready = norm_channels(flat, gain[...]).astype(jnp.bfloat16)
    out[...] = jax.nn.sigmoid(dot(ready, weight[...])).reshape(rows, columns, -1)


def add_block(left, right, sums, place):
    depth, columns, width = right.shape
    half = left.shape[0] // depth
    group = max(g for g in range(1, half + 1) if half % g == 0 and g * columns <= 288)
    for base in range(0, half, group):

        def step(k, totals):
            line = right[k]
            return tuple(
                total + left[pl.ds(k * half + base + i, 1)] * line
                for i, total in enumerate(totals)
            )

        totals = (jnp.zeros((columns, width), jnp.float32),) * group
        totals = lax.fori_loop(0, depth, step, totals, unroll=6)
        for i, total in enumerate(totals):
            sums[place, base + i] = total


def first_kernel(kept, mine, other, gain, left_weight, right_weight, right, sums, left):
    rows, columns, width = mine.shape
    for part, block in enumerate((mine, other)):
        flat = project(block[...].reshape(rows * columns, width), gain[...], right_weight[...])
        right[pl.ds(part * rows, rows)] = flat.reshape(rows, columns, -1)
    left[...] = project(kept[...], gain[...], left_weight[...])
    add_block(left, right, sums, lax.axis_index("second"))


def middle_kernel(steps, *refs):
    (right, gain, weight, _, sums, left) = refs[len(steps) :]
    for step, block in zip(steps, refs):
        left[...] = project(block[...], gain[...], weight[...])
        add_block(left, right, sums, lax.axis_index("second") ^ step)


def last_kernel(step, messages, merge, block, right, gain, weight, before, *refs):
    *outs, sums, left = refs
    first, second = lax.axis_index("first"), lax.axis_index("second")
    chip, core = first // 2, lax.rem(first, 2)
    left[...] = project(block[...], gain[...], weight[...])
    add_block(left, right, sums, second ^ step)
    for out, (chips, cores) in zip(outs, messages):
        place = (chip ^ chips) if merge == 1 else 2 * (chip ^ chips) + (core ^ cores)
        out[...] = sums[place].astype(out.dtype)


def final_kernel(merge, per, scale, *refs):
    parts, (gate, gain, weight, out) = refs[:-4], refs[-4:]
    core = core_of()
    half, columns, width = parts[0].shape
    for slot in range(merge):
        mine = parts[slot * per : (slot + 1) * per]
        total = sum(part[...].astype(jnp.float32) for part in mine)
        flat = total.reshape(half * columns, width) * scale
        scaled = norm_channels(flat, gain[...]).astype(jnp.bfloat16)
        result = dot(scaled, weight[...]).reshape(half, columns, -1)
        rows = pl.ds(0, half) if merge == 1 else pl.ds((core ^ slot) * half, half)
        out[rows] = (result * gate[rows]).astype(out.dtype)


def call(kernel, out_shapes, *operands, scratch=(), waits=(), flops=0, aliases={}, space=pltpu.VMEM):
    many = isinstance(out_shapes, list)
    held = jax.tree.leaves(out_shapes) + list(operands) + list(scratch)
    held = sum(math.prod(ref.shape) * jnp.dtype(ref.dtype).itemsize for ref in held)
    return pl.pallas_call(
        kernel,
        out_shape=out_shapes,
        in_specs=[pl.BlockSpec(memory_space=space)] * len(operands),
        out_specs=[VMEM] * len(out_shapes) if many else VMEM,
        scratch_shapes=[*scratch, *waits],
        input_output_aliases=aliases,
        compiler_params=pltpu.CompilerParams(vmem_limit_bytes=held + (2 << 20)),
        cost_estimate=pl.CostEstimate(flops=flops, bytes_accessed=100000, transcendentals=0),
    )(*operands)


def shards(pair_rows, in_gain, left_weight, right_weight, mid_gain, out_weight, out_gate):
    firsts, seconds = lax.axis_size("first"), lax.axis_size("second")
    rows, columns, width = pair_rows.shape
    mix, wide = left_weight.shape[1], out_weight.shape[1]
    chips, half, depth = firsts // 2, columns // 2, 2 * rows
    merge = rows // half
    in_gain, mid_gain = in_gain.reshape(1, -1), mid_gain.reshape(1, -1)
    axes = ("first", "second")
    shape, f32 = jax.ShapeDtypeStruct, jnp.float32

    def swap(values, chip=0, core=0, block=0):
        pairs = [
            (a * seconds + b, (a ^ (2 * chip + core)) * seconds + (b ^ block))
            for a in range(firsts)
            for b in range(seconds)
        ]
        return lax.ppermute(values, axes, pairs)

    work = 2 * depth * half * width * mix
    lefts = [pltpu.VMEM((depth * half, mix), f32)]
    held = shape((seconds, half, columns, mix), f32)
    other = swap(pair_rows, core=1)
    arguments = (
        pair_rows,
        in_gain,
        right_weight,
        out_gate,
        left_weight,
        mid_gain,
        out_weight,
    )
    mine, in_gain, right_weight, out_gate, left_weight, mid_gain, out_weight = call(
        load_kernel,
        [shape(x.shape, x.dtype) for x in arguments],
        *[pltpu.with_memory_space_constraint(x, pltpu.HBM) for x in arguments],
        waits=[pltpu.SemaphoreType.DMA((len(arguments),))],
        space=pltpu.HBM,
    )
    kept = call(
        pack_kernel,
        shape((depth * half, width), pair_rows.dtype),
        mine,
        other,
        scratch=[pltpu.VMEM((depth * half, width), f32)],
    )
    nears = [1, 2, 3] if seconds == 4 else list(range(1, seconds))
    blocks = [swap(kept, block=s) for s in nears]
    right, sums = call(
        first_kernel,
        [shape((depth, columns, mix), f32), held],
        kept,
        mine,
        other,
        in_gain,
        left_weight,
        right_weight,
        scratch=lefts,
        flops=10 * work,
    )
    factors = (right, in_gain, left_weight)
    sums = call(
        functools.partial(middle_kernel, nears[:-1]),
        held,
        *blocks[:-1],
        *factors,
        sums,
        scratch=lefts,
        flops=10 * (seconds - 2) * work,
        aliases={seconds + 1: 0},
    )
    cores = range(merge)
    order = [3, 1, 2] if chips == 4 else list(range(1, chips))
    messages = [(t, c) for t in order + [0] for c in reversed(cores)]
    *outgoing, _ = call(
        functools.partial(last_kernel, nears[-1], messages, merge),
        [shape((half, columns, mix), f32 if m == (0, 0) else jnp.bfloat16) for m in messages]
        + [held],
        blocks[-1],
        *factors,
        sums,
        scratch=lefts,
        flops=10 * work,
        aliases={4: len(messages)},
    )
    gate = call(
        gate_kernel,
        shape((rows, columns, wide), f32),
        mine,
        in_gain,
        out_gate,
        flops=2 * rows * columns * width * wide,
    )
    arrived = {
        (t, c): part if (t, c) == (0, 0) else swap(part, chip=t, core=c)
        for (t, c), part in zip(messages, outgoing)
    }
    parts = [arrived[t, c] for c in cores for t in [0] + order]
    return call(
        functools.partial(final_kernel, merge, chips, (rows * firsts) ** -0.5),
        shape((rows, columns, wide), jnp.bfloat16),
        *parts,
        gate,
        mid_gain,
        out_weight,
        flops=2 * rows * columns * mix * wide,
    )


def solution(mesh):
    in_specs = (P("first", "second", None), P(), P(), P(), P(), P(), P())
    out_specs = P("first", "second", None)
    return jax.shard_map(shards, mesh=mesh, in_specs=in_specs, out_specs=out_specs, check_vma=False)
```

```python
import functools
import math

import jax
import jax.numpy as jnp
from jax import lax
from jax.experimental import pallas as pl
from jax.experimental.pallas import tpu as pltpu
from jax.sharding import PartitionSpec as P


EARLY, LATE, ORDER = 1, [2, 3], [3, 1, 2]
VMEM = pl.BlockSpec(memory_space=pltpu.VMEM)


def norm_channels(values, channel_gain):
    centred = values - jnp.mean(values, axis=-1, keepdims=True)
    variance = jnp.mean(centred * centred, axis=-1, keepdims=True)
    return centred * lax.rsqrt(variance + 1e-05) * channel_gain


def dot(rows, weight):
    return jnp.dot(rows, weight, preferred_element_type=jnp.float32)


def project(rows, gain, weight):
    ready = norm_channels(rows.astype(jnp.float32), gain).astype(jnp.bfloat16)
    return dot(ready, weight).astype(jnp.bfloat16).astype(jnp.float32)


def core_of():
    return lax.rem(lax.axis_index("first"), 2)


def cut(block, upper, flat, at):
    half = block.shape[1] // 2
    for k in range(block.shape[0]):
        row = block[k].astype(jnp.float32)
        flat[pl.ds(at + k * half, half)] = jnp.where(upper, row[half:], row[:half])


def pack_kernel(mine, other, out, flat):
    upper = core_of() == 1
    cut(mine, upper, flat, 0)
    cut(other, upper, flat, flat.shape[0] // 2)
    out[...] = flat[...].astype(out.dtype)


def split_kernel(block, kept, passed, flat):
    cut(block, core_of() == 1, flat, 0)
    kept[...] = flat[...].astype(kept.dtype)
    cut(block, core_of() == 0, flat, 0)
    passed[...] = flat[...].astype(passed.dtype)


def load_kernel(*refs):
    count = len(refs) // 2
    copies = [
        pltpu.make_async_copy(source, target, refs[-1].at[i])
        for i, (source, target) in enumerate(zip(refs[:count], refs[count:-1]))
    ]
    for copy in copies:
        copy.start()
    for copy in copies:
        copy.wait()


def gate_kernel(mine, gain, weight, out):
    rows, columns, width = mine.shape
    flat = mine[...].reshape(rows * columns, width).astype(jnp.float32)
    ready = norm_channels(flat, gain[...]).astype(jnp.bfloat16)
    out[...] = jax.nn.sigmoid(dot(ready, weight[...])).reshape(rows, columns, -1)


def add_block(left, right, sums, place):
    depth, columns, width = right.shape
    half = left.shape[0] // depth
    group = max(g for g in range(1, half + 1) if half % g == 0 and g * columns <= 288)
    for base in range(0, half, group):

        def step(k, totals):
            line = right[k]
            return tuple(
                total + left[pl.ds(k * half + base + i, 1)] * line
                for i, total in enumerate(totals)
            )

        totals = (jnp.zeros((columns, width), jnp.float32),) * group
        totals = lax.fori_loop(0, depth, step, totals, unroll=6)
        for i, total in enumerate(totals):
            sums[place, base + i] = total


def first_kernel(kept, mine, other, gain, left_weight, right_weight, right, sums, left):
    rows, columns, width = mine.shape
    for part, block in enumerate((mine, other)):
        flat = project(block[...].reshape(rows * columns, width), gain[...], right_weight[...])
        right[pl.ds(part * rows, rows)] = flat.reshape(rows, columns, -1)
    left[...] = project(kept[...], gain[...], left_weight[...])
    add_block(left, right, sums, lax.axis_index("second"))


def middle_kernel(steps, *refs):
    (right, gain, weight, _, sums, left) = refs[len(steps) :]
    for step, block in zip(steps, refs):
        left[...] = project(block[...], gain[...], weight[...])
        add_block(left, right, sums, lax.axis_index("second") ^ step)


def joined_kernel(step, kept, passed, right, gain, weight, _, sums, left):
    rows = kept.shape[0]
    for part, block in enumerate((kept, passed)):
        left[pl.ds(part * rows, rows)] = project(block[...], gain[...], weight[...])
    add_block(left, right, sums, lax.axis_index("second") ^ step)


def last_kernel(step, messages, merge, block, right, gain, weight, before, *refs):
    *outs, sums, left = refs
    first, second = lax.axis_index("first"), lax.axis_index("second")
    chip, core = first // 2, lax.rem(first, 2)
    left[...] = project(block[...], gain[...], weight[...])
    add_block(left, right, sums, second ^ step)
    for out, (chips, cores) in zip(outs, messages):
        place = (chip ^ chips) if merge == 1 else 2 * (chip ^ chips) + (core ^ cores)
        out[...] = sums[place].astype(out.dtype)


def final_kernel(merge, per, scale, *refs):
    parts, (gate, gain, weight, out) = refs[:-4], refs[-4:]
    core = core_of()
    half, columns, width = parts[0].shape
    for slot in range(merge):
        mine = parts[slot * per : (slot + 1) * per]
        total = sum(part[...].astype(jnp.float32) for part in mine)
        flat = total.reshape(half * columns, width) * scale
        scaled = norm_channels(flat, gain[...]).astype(jnp.bfloat16)
        result = dot(scaled, weight[...]).reshape(half, columns, -1)
        rows = pl.ds(0, half) if merge == 1 else pl.ds((core ^ slot) * half, half)
        out[rows] = (result * gate[rows]).astype(out.dtype)


def call(kernel, out_shapes, *operands, scratch=(), waits=(), aliases={}, space=pltpu.VMEM):
    many = isinstance(out_shapes, list)
    held = jax.tree.leaves(out_shapes) + list(operands) + list(scratch)
    held = sum(math.prod(ref.shape) * jnp.dtype(ref.dtype).itemsize for ref in held)
    return pl.pallas_call(
        kernel,
        out_shape=out_shapes,
        in_specs=[pl.BlockSpec(memory_space=space)] * len(operands),
        out_specs=[VMEM] * len(out_shapes) if many else VMEM,
        scratch_shapes=[*scratch, *waits],
        input_output_aliases=aliases,
        compiler_params=pltpu.CompilerParams(vmem_limit_bytes=held + (2 << 20)),
        cost_estimate=pl.CostEstimate(
            flops=1 << 24, bytes_accessed=100000, transcendentals=0
        ),
    )(*operands)


def shards(pair_rows, in_gain, left_weight, right_weight, mid_gain, out_weight, out_gate):
    firsts, seconds = lax.axis_size("first"), lax.axis_size("second")
    rows, columns, width = pair_rows.shape
    mix, wide = left_weight.shape[1], out_weight.shape[1]
    chips, half, depth = firsts // 2, columns // 2, 2 * rows
    merge = rows // half
    in_gain, mid_gain = in_gain.reshape(1, -1), mid_gain.reshape(1, -1)
    axes = ("first", "second")
    shape, f32 = jax.ShapeDtypeStruct, jnp.float32

    def swap(values, chip=0, core=0, block=0):
        pairs = [
            (a * seconds + b, (a ^ (2 * chip + core)) * seconds + (b ^ block))
            for a in range(firsts)
            for b in range(seconds)
        ]
        return lax.ppermute(values, axes, pairs)

    lefts = [pltpu.VMEM((depth * half, mix), f32)]
    held = shape((seconds, half, columns, mix), f32)
    flat = shape((depth * half, width), pair_rows.dtype)
    part = shape((rows * half, width), pair_rows.dtype)
    other = swap(pair_rows, core=1)
    early = swap(pair_rows, block=EARLY)
    arguments = (
        pair_rows,
        in_gain,
        right_weight,
        out_gate,
        left_weight,
        mid_gain,
        out_weight,
    )
    mine, in_gain, right_weight, out_gate, left_weight, mid_gain, out_weight = call(
        load_kernel,
        [shape(x.shape, x.dtype) for x in arguments],
        *[pltpu.with_memory_space_constraint(x, pltpu.HBM) for x in arguments],
        waits=[pltpu.SemaphoreType.DMA((len(arguments),))],
        space=pltpu.HBM,
    )
    kept = call(pack_kernel, flat, mine, other, scratch=[pltpu.VMEM(flat.shape, f32)])
    late = [s for s in range(1, seconds) if s != EARLY]
    if seconds == 4:
        late = LATE
    blocks = [swap(kept, block=s) for s in late[:-1]]
    last = swap(kept, block=late[-1])
    right, sums = call(
        first_kernel,
        [shape((depth, columns, mix), f32), held],
        kept,
        mine,
        other,
        in_gain,
        left_weight,
        right_weight,
        scratch=lefts,
    )
    factors = (right, in_gain, left_weight)
    near, passed = call(split_kernel, [part, part], early, scratch=[pltpu.VMEM(part.shape, f32)])
    passed = swap(passed, core=1)
    sums = call(
        functools.partial(middle_kernel, late[:-1]),
        held,
        *blocks,
        *factors,
        sums,
        scratch=lefts,
        aliases={len(blocks) + 3: 0},
    )
    sums = call(
        functools.partial(joined_kernel, EARLY),
        held,
        near,
        passed,
        *factors,
        sums,
        scratch=lefts,
        aliases={5: 0},
    )
    cores = range(merge)
    order = ORDER if chips == 4 else list(range(1, chips))
    messages = [(t, c) for t in order + [0] for c in reversed(cores)]
    *outgoing, _ = call(
        functools.partial(last_kernel, late[-1], messages, merge),
        [shape((half, columns, mix), f32 if m == (0, 0) else jnp.bfloat16) for m in messages]
        + [held],
        last,
        *factors,
        sums,
        scratch=lefts,
        aliases={4: len(messages)},
    )
    gate = call(gate_kernel, shape((rows, columns, wide), f32), mine, in_gain, out_gate)
    arrived = {
        (t, c): sent if (t, c) == (0, 0) else swap(sent, chip=t, core=c)
        for (t, c), sent in zip(messages, outgoing)
    }
    parts = [arrived[t, c] for c in cores for t in [0] + order]
    return call(
        functools.partial(final_kernel, merge, chips, (rows * firsts) ** -0.5),
        shape((rows, columns, wide), jnp.bfloat16),
        *parts,
        gate,
        mid_gain,
        out_weight,
    )


def solution(mesh):
    in_specs = (P("first", "second", None), P(), P(), P(), P(), P(), P())
    out_specs = P("first", "second", None)
    return jax.shard_map(shards, mesh=mesh, in_specs=in_specs, out_specs=out_specs, check_vma=False)
```

```python
import functools
import math

import jax
import jax.numpy as jnp
from jax import lax
from jax.experimental import pallas as pl
from jax.experimental.pallas import tpu as pltpu
from jax.sharding import PartitionSpec as P


EARLY, LATE, ORDER = 3, [1, 2], [2, 3, 1]
VMEM = pl.BlockSpec(memory_space=pltpu.VMEM)


def norm_channels(values, channel_gain):
    centred = values - jnp.mean(values, axis=-1, keepdims=True)
    variance = jnp.mean(centred * centred, axis=-1, keepdims=True)
    return centred * lax.rsqrt(variance + 1e-05) * channel_gain


def dot(rows, weight):
    return jnp.dot(rows, weight, preferred_element_type=jnp.float32)


def project(rows, gain, weight):
    ready = norm_channels(rows.astype(jnp.float32), gain).astype(jnp.bfloat16)
    return dot(ready, weight).astype(jnp.bfloat16).astype(jnp.float32)


def core_of():
    return lax.rem(lax.axis_index("first"), 2)


def cut(block, upper, flat, at):
    half = block.shape[1] // 2
    for k in range(block.shape[0]):
        row = block[k].astype(jnp.float32)
        flat[pl.ds(at + k * half, half)] = jnp.where(upper, row[half:], row[:half])


def pack_kernel(mine, other, gain, weight, out, flat):
    upper = core_of() == 1
    cut(mine, upper, flat, 0)
    cut(other, upper, flat, flat.shape[0] // 2)
    out[...] = project(flat[...], gain[...], weight[...]).astype(out.dtype)


def split_kernel(block, kept, passed, flat):
    cut(block, core_of() == 1, flat, 0)
    kept[...] = flat[...].astype(kept.dtype)
    cut(block, core_of() == 0, flat, 0)
    passed[...] = flat[...].astype(passed.dtype)


def load_kernel(*refs):
    count = len(refs) // 2
    copies = [
        pltpu.make_async_copy(source, target, refs[-1].at[i])
        for i, (source, target) in enumerate(zip(refs[:count], refs[count:-1]))
    ]
    for copy in copies:
        copy.start()
    for copy in copies:
        copy.wait()


def gate_kernel(mine, gain, weight, out):
    rows, columns, width = mine.shape
    flat = mine[...].reshape(rows * columns, width).astype(jnp.float32)
    ready = norm_channels(flat, gain[...]).astype(jnp.bfloat16)
    out[...] = jax.nn.sigmoid(dot(ready, weight[...])).reshape(rows, columns, -1)


def add_block(left, right, sums, place):
    depth, columns, width = right.shape
    half = left.shape[0] // depth
    group = max(g for g in range(1, half + 1) if half % g == 0 and g * columns <= 288)
    for base in range(0, half, group):

        def step(k, totals):
            line = right[k]
            return tuple(
                total + left[pl.ds(k * half + base + i, 1)] * line
                for i, total in enumerate(totals)
            )

        totals = (jnp.zeros((columns, width), jnp.float32),) * group
        totals = lax.fori_loop(0, depth, step, totals, unroll=6)
        for i, total in enumerate(totals):
            sums[place, base + i] = total


def first_kernel(kept, mine, other, gain, right_weight, right, sums, left):
    rows, columns, width = mine.shape
    for part, block in enumerate((mine, other)):
        flat = project(block[...].reshape(rows * columns, width), gain[...], right_weight[...])
        right[pl.ds(part * rows, rows)] = flat.reshape(rows, columns, -1)
    left[...] = kept[...].astype(jnp.float32)
    add_block(left, right, sums, lax.axis_index("second"))


def middle_kernel(steps, *refs):
    (right, _, sums, left) = refs[len(steps) :]
    for step, block in zip(steps, refs):
        left[...] = block[...].astype(jnp.float32)
        add_block(left, right, sums, lax.axis_index("second") ^ step)


def joined_kernel(step, kept, passed, right, gain, weight, _, sums, left):
    rows = kept.shape[0]
    for part, block in enumerate((kept, passed)):
        left[pl.ds(part * rows, rows)] = project(block[...], gain[...], weight[...])
    add_block(left, right, sums, lax.axis_index("second") ^ step)


def last_kernel(step, messages, merge, block, right, before, *refs):
    *outs, sums, left = refs
    first, second = lax.axis_index("first"), lax.axis_index("second")
    chip, core = first // 2, lax.rem(first, 2)
    left[...] = block[...].astype(jnp.float32)
    add_block(left, right, sums, second ^ step)
    for out, (chips, cores) in zip(outs, messages):
        place = (chip ^ chips) if merge == 1 else 2 * (chip ^ chips) + (core ^ cores)
        out[...] = sums[place].astype(out.dtype)


def final_kernel(merge, per, scale, *refs):
    parts, (gate, gain, weight, out) = refs[:-4], refs[-4:]
    core = core_of()
    half, columns, width = parts[0].shape
    for slot in range(merge):
        mine = parts[slot * per : (slot + 1) * per]
        total = sum(part[...].astype(jnp.float32) for part in mine)
        flat = total.reshape(half * columns, width) * scale
        scaled = norm_channels(flat, gain[...]).astype(jnp.bfloat16)
        result = dot(scaled, weight[...]).reshape(half, columns, -1)
        rows = pl.ds(0, half) if merge == 1 else pl.ds((core ^ slot) * half, half)
        out[rows] = (result * gate[rows]).astype(out.dtype)


def call(kernel, out_shapes, *operands, scratch=(), waits=(), aliases={}, space=pltpu.VMEM):
    many = isinstance(out_shapes, list)
    held = jax.tree.leaves(out_shapes) + list(operands) + list(scratch)
    held = sum(math.prod(ref.shape) * jnp.dtype(ref.dtype).itemsize for ref in held)
    return pl.pallas_call(
        kernel,
        out_shape=out_shapes,
        in_specs=[pl.BlockSpec(memory_space=space)] * len(operands),
        out_specs=[VMEM] * len(out_shapes) if many else VMEM,
        scratch_shapes=[*scratch, *waits],
        input_output_aliases=aliases,
        compiler_params=pltpu.CompilerParams(vmem_limit_bytes=held + (2 << 20)),
        cost_estimate=pl.CostEstimate(
            flops=1 << 24, bytes_accessed=100000, transcendentals=0
        ),
    )(*operands)


def shards(pair_rows, in_gain, left_weight, right_weight, mid_gain, out_weight, out_gate):
    firsts, seconds = lax.axis_size("first"), lax.axis_size("second")
    rows, columns, width = pair_rows.shape
    mix, wide = left_weight.shape[1], out_weight.shape[1]
    chips, half, depth = firsts // 2, columns // 2, 2 * rows
    merge = rows // half
    in_gain, mid_gain = in_gain.reshape(1, -1), mid_gain.reshape(1, -1)
    axes = ("first", "second")
    shape, f32 = jax.ShapeDtypeStruct, jnp.float32

    def swap(values, chip=0, core=0, block=0):
        pairs = [
            (a * seconds + b, (a ^ (2 * chip + core)) * seconds + (b ^ block))
            for a in range(firsts)
            for b in range(seconds)
        ]
        return lax.ppermute(values, axes, pairs)

    lefts = [pltpu.VMEM((depth * half, mix), f32)]
    held = shape((seconds, half, columns, mix), f32)
    part = shape((rows * half, width), pair_rows.dtype)
    other = swap(pair_rows, core=1)
    early = swap(pair_rows, block=EARLY)
    arguments = (
        pair_rows,
        in_gain,
        right_weight,
        out_gate,
        left_weight,
        mid_gain,
        out_weight,
    )
    mine, in_gain, right_weight, out_gate, left_weight, mid_gain, out_weight = call(
        load_kernel,
        [shape(x.shape, x.dtype) for x in arguments],
        *[pltpu.with_memory_space_constraint(x, pltpu.HBM) for x in arguments],
        waits=[pltpu.SemaphoreType.DMA((len(arguments),))],
        space=pltpu.HBM,
    )
    kept = call(
        pack_kernel,
        shape((depth * half, mix), jnp.bfloat16),
        mine,
        other,
        in_gain,
        left_weight,
        scratch=[pltpu.VMEM((depth * half, width), f32)],
    )
    late = [s for s in range(1, seconds) if s != EARLY]
    if seconds == 4:
        late = LATE
    blocks = [swap(kept, block=s) for s in late[:-1]]
    last = swap(kept, block=late[-1])
    right, sums = call(
        first_kernel,
        [shape((depth, columns, mix), f32), held],
        kept,
        mine,
        other,
        in_gain,
        right_weight,
        scratch=lefts,
    )
    factors = (right, in_gain, left_weight)
    near, passed = call(split_kernel, [part, part], early, scratch=[pltpu.VMEM(part.shape, f32)])
    passed = swap(passed, core=1)
    sums = call(
        functools.partial(joined_kernel, EARLY),
        held,
        near,
        passed,
        *factors,
        sums,
        scratch=lefts,
        aliases={5: 0},
    )
    sums = call(
        functools.partial(middle_kernel, late[:-1]),
        held,
        *blocks,
        right,
        sums,
        scratch=lefts,
        aliases={len(blocks) + 1: 0},
    )
    cores = range(merge)
    order = ORDER if chips == 4 else list(range(1, chips))
    messages = [(t, c) for t in order + [0] for c in reversed(cores)]
    *outgoing, _ = call(
        functools.partial(last_kernel, late[-1], messages, merge),
        [shape((half, columns, mix), f32 if m == (0, 0) else jnp.bfloat16) for m in messages]
        + [held],
        last,
        right,
        sums,
        scratch=lefts,
        aliases={2: len(messages)},
    )
    gate = call(gate_kernel, shape((rows, columns, wide), f32), mine, in_gain, out_gate)
    arrived = {
        (t, c): sent if (t, c) == (0, 0) else swap(sent, chip=t, core=c)
        for (t, c), sent in zip(messages, outgoing)
    }
    parts = [arrived[t, c] for c in cores for t in [0] + order]
    return call(
        functools.partial(final_kernel, merge, chips, (rows * firsts) ** -0.5),
        shape((rows, columns, wide), jnp.bfloat16),
        *parts,
        gate,
        mid_gain,
        out_weight,
    )


def solution(mesh):
    in_specs = (P("first", "second", None), P(), P(), P(), P(), P(), P())
    out_specs = P("first", "second", None)
    return jax.shard_map(shards, mesh=mesh, in_specs=in_specs, out_specs=out_specs, check_vma=False)
```

```python
import functools
import math

import jax
import jax.numpy as jnp
from jax import lax
from jax.experimental import pallas as pl
from jax.experimental.pallas import tpu as pltpu
from jax.sharding import PartitionSpec as P


VMEM = pl.BlockSpec(memory_space=pltpu.VMEM)


def norm_channels(values, channel_gain):
    centred = values - jnp.mean(values, axis=-1, keepdims=True)
    variance = jnp.mean(centred * centred, axis=-1, keepdims=True)
    return centred * lax.rsqrt(variance + 1e-05) * channel_gain


def dot(rows, weight):
    return jnp.dot(rows, weight, preferred_element_type=jnp.float32)


def project(rows, gain, weight):
    ready = norm_channels(rows.astype(jnp.float32), gain).astype(jnp.bfloat16)
    return dot(ready, weight).astype(jnp.bfloat16).astype(jnp.float32)


def core_of():
    return lax.rem(lax.axis_index("first"), 2)


def cut(block, upper, flat, at):
    half = block.shape[1] // 2
    for k in range(block.shape[0]):
        row = block[k].astype(jnp.float32)
        flat[pl.ds(at + k * half, half)] = jnp.where(upper, row[half:], row[:half])


def pack_kernel(mine, other, gain, weight, out, flat):
    upper = core_of() == 1
    cut(mine, upper, flat, 0)
    cut(other, upper, flat, flat.shape[0] // 2)
    out[...] = project(flat[...], gain[...], weight[...]).astype(out.dtype)


def split_kernel(block, kept, passed, flat):
    cut(block, core_of() == 1, flat, 0)
    kept[...] = flat[...].astype(kept.dtype)
    cut(block, core_of() == 0, flat, 0)
    passed[...] = flat[...].astype(passed.dtype)


def load_kernel(*refs):
    count = len(refs) // 2
    copies = [
        pltpu.make_async_copy(source, target, refs[-1].at[i])
        for i, (source, target) in enumerate(zip(refs[:count], refs[count:-1]))
    ]
    for copy in copies:
        copy.start()
    for copy in copies:
        copy.wait()


def gate_kernel(mine, gain, weight, out):
    rows, columns, width = mine.shape
    flat = mine[...].reshape(rows * columns, width).astype(jnp.float32)
    ready = norm_channels(flat, gain[...]).astype(jnp.bfloat16)
    out[...] = jax.nn.sigmoid(dot(ready, weight[...])).reshape(rows, columns, -1)


def add_block(left, right, sums, place, start=0, more=False):
    _, half, columns, width = sums.shape
    depth = left.shape[0] // half
    group = max(g for g in range(1, half + 1) if half % g == 0 and g * columns <= 288)
    for base in range(0, half, group):

        def step(k, totals):
            line = right[start + k]
            return tuple(
                total + left[pl.ds(k * half + base + i, 1)] * line
                for i, total in enumerate(totals)
            )

        totals = (jnp.zeros((columns, width), jnp.float32),) * group
        if more:
            totals = tuple(sums[place, base + i] for i in range(group))
        totals = lax.fori_loop(0, depth, step, totals, unroll=6)
        for i, total in enumerate(totals):
            sums[place, base + i] = total


def first_kernel(kept, mine, other, gain, right_weight, right, sums, left):
    rows, columns, width = mine.shape
    for part, block in enumerate((mine, other)):
        flat = project(block[...].reshape(rows * columns, width), gain[...], right_weight[...])
        right[pl.ds(part * rows, rows)] = flat.reshape(rows, columns, -1)
    left[...] = kept[...].astype(jnp.float32)
    add_block(left, right, sums, lax.axis_index("second"))


def middle_kernel(steps, *refs):
    (right, _, sums, left) = refs[len(steps) :]
    for step, block in zip(steps, refs):
        left[...] = block[...].astype(jnp.float32)
        add_block(left, right, sums, lax.axis_index("second") ^ step)


def part_kernel(step, more, block, right, gain, weight, _, sums, left):
    left[...] = project(block[...], gain[...], weight[...])
    start = right.shape[0] // 2 if more else 0
    add_block(left, right, sums, lax.axis_index("second") ^ step, start, more)


def last_kernel(step, messages, merge, block, right, before, *refs):
    *outs, sums, left = refs
    first, second = lax.axis_index("first"), lax.axis_index("second")
    chip, core = first // 2, lax.rem(first, 2)
    left[...] = block[...].astype(jnp.float32)
    add_block(left, right, sums, second ^ step)
    for out, (targets, cores) in zip(outs, messages):
        place = jnp.int32(0)
        for z, target in enumerate(targets):
            place = jnp.where(chip == z, target, place)
        place = place if merge == 1 else 2 * place + (core ^ cores)
        out[...] = sums[place].astype(out.dtype)


def final_kernel(merge, per, scale, *refs):
    parts, (gate, gain, weight, out) = refs[:-4], refs[-4:]
    core = core_of()
    half, columns, width = parts[0].shape
    for slot in range(merge):
        mine = parts[slot * per : (slot + 1) * per]
        total = sum(part[...].astype(jnp.float32) for part in mine)
        flat = total.reshape(half * columns, width) * scale
        scaled = norm_channels(flat, gain[...]).astype(jnp.bfloat16)
        result = dot(scaled, weight[...]).reshape(half, columns, -1)
        rows = pl.ds(0, half) if merge == 1 else pl.ds((core ^ slot) * half, half)
        out[rows] = (result * gate[rows]).astype(out.dtype)


def call(kernel, out_shapes, *operands, scratch=(), waits=(), aliases={}, space=pltpu.VMEM):
    many = isinstance(out_shapes, list)
    held = jax.tree.leaves(out_shapes) + list(operands) + list(scratch)
    held = sum(math.prod(ref.shape) * jnp.dtype(ref.dtype).itemsize for ref in held)
    return pl.pallas_call(
        kernel,
        out_shape=out_shapes,
        in_specs=[pl.BlockSpec(memory_space=space)] * len(operands),
        out_specs=[VMEM] * len(out_shapes) if many else VMEM,
        scratch_shapes=[*scratch, *waits],
        input_output_aliases=aliases,
        compiler_params=pltpu.CompilerParams(vmem_limit_bytes=held + (2 << 20)),
        cost_estimate=pl.CostEstimate(
            flops=1 << 24, bytes_accessed=100000, transcendentals=0
        ),
    )(*operands)


def shards(pair_rows, in_gain, left_weight, right_weight, mid_gain, out_weight, out_gate):
    firsts, seconds = lax.axis_size("first"), lax.axis_size("second")
    rows, columns, width = pair_rows.shape
    mix, wide = left_weight.shape[1], out_weight.shape[1]
    chips, half, depth = firsts // 2, columns // 2, 2 * rows
    merge = rows // half
    in_gain, mid_gain = in_gain.reshape(1, -1), mid_gain.reshape(1, -1)
    axes = ("first", "second")
    shape, f32 = jax.ShapeDtypeStruct, jnp.float32

    ring = [0, *range(1, chips, 2), *range(2, chips, 2)[::-1]]
    targets = [
        [ring[(ring.index(z) + step) % chips] for z in range(chips)] for step in range(chips)
    ]

    def swap(values, step=0, core=0, block=0):
        pairs = [
            (a * seconds + b, (2 * targets[step][a // 2] + (a % 2 ^ core)) * seconds + (b ^ block))
            for a in range(firsts)
            for b in range(seconds)
        ]
        return lax.ppermute(values, axes, pairs)

    lefts = [pltpu.VMEM((depth * half, mix), f32)]
    held = shape((seconds, half, columns, mix), f32)
    part = shape((rows * half, width), pair_rows.dtype)
    other = swap(pair_rows, core=1)
    early = swap(pair_rows, block=seconds - 1)
    arguments = (
        pair_rows,
        in_gain,
        right_weight,
        out_gate,
        left_weight,
        mid_gain,
        out_weight,
    )
    mine, in_gain, right_weight, out_gate, left_weight, mid_gain, out_weight = call(
        load_kernel,
        [shape(x.shape, x.dtype) for x in arguments],
        *[pltpu.with_memory_space_constraint(x, pltpu.HBM) for x in arguments],
        waits=[pltpu.SemaphoreType.DMA((len(arguments),))],
        space=pltpu.HBM,
    )
    kept = call(
        pack_kernel,
        shape((depth * half, mix), jnp.bfloat16),
        mine,
        other,
        in_gain,
        left_weight,
        scratch=[pltpu.VMEM((depth * half, width), f32)],
    )
    late = list(range(1, seconds - 1))
    blocks = [swap(kept, block=s) for s in late[:-1]]
    last = swap(kept, block=late[-1])
    right, sums = call(
        first_kernel,
        [shape((depth, columns, mix), f32), held],
        kept,
        mine,
        other,
        in_gain,
        right_weight,
        scratch=lefts,
    )
    factors = (right, in_gain, left_weight)
    near, passed = call(split_kernel, [part, part], early, scratch=[pltpu.VMEM(part.shape, f32)])
    passed = swap(passed, core=1)
    for block, more in ((near, False), (passed, True)):
        sums = call(
            functools.partial(part_kernel, seconds - 1, more),
            held,
            block,
            *factors,
            sums,
            scratch=[pltpu.VMEM((rows * half, mix), f32)],
            aliases={4: 0},
        )
    sums = call(
        functools.partial(middle_kernel, late[:-1]),
        held,
        *blocks,
        right,
        sums,
        scratch=lefts,
        aliases={len(blocks) + 1: 0},
    )
    cores = range(merge)
    messages = [(t, c) for t in [*range(1, chips), 0] for c in reversed(cores)]
    *outgoing, _ = call(
        functools.partial(
            last_kernel, late[-1], [(targets[t], c) for t, c in messages], merge
        ),
        [shape((half, columns, mix), f32 if m == (0, 0) else jnp.bfloat16) for m in messages]
        + [held],
        last,
        right,
        sums,
        scratch=lefts,
        aliases={2: len(messages)},
    )
    gate = call(gate_kernel, shape((rows, columns, wide), f32), mine, in_gain, out_gate)
    arrived = {
        (t, c): sent if (t, c) == (0, 0) else swap(sent, step=t, core=c)
        for (t, c), sent in zip(messages, outgoing)
    }
    parts = [arrived[t, c] for c in cores for t in range(chips)]
    return call(
        functools.partial(final_kernel, merge, chips, (rows * firsts) ** -0.5),
        shape((rows, columns, wide), jnp.bfloat16),
        *parts,
        gate,
        mid_gain,
        out_weight,
    )


def solution(mesh):
    in_specs = (P("first", "second", None), P(), P(), P(), P(), P(), P())
    out_specs = P("first", "second", None)
    return jax.shard_map(shards, mesh=mesh, in_specs=in_specs, out_specs=out_specs, check_vma=False)
```

```python
import functools
import math

import jax
import jax.numpy as jnp
from jax import lax
from jax.experimental import pallas as pl
from jax.experimental.pallas import tpu as pltpu
from jax.sharding import PartitionSpec as P


VMEM = pl.BlockSpec(memory_space=pltpu.VMEM)


def norm_channels(values, channel_gain):
    centred = values - jnp.mean(values, axis=-1, keepdims=True)
    variance = jnp.mean(centred * centred, axis=-1, keepdims=True)
    return centred * lax.rsqrt(variance + 1e-05) * channel_gain


def dot(rows, weight):
    return jnp.dot(rows, weight, preferred_element_type=jnp.float32)


def project(rows, gain, weight):
    ready = norm_channels(rows.astype(jnp.float32), gain).astype(jnp.bfloat16)
    return dot(ready, weight).astype(jnp.bfloat16).astype(jnp.float32)


def core_of():
    return lax.rem(lax.axis_index("first"), 2)


def cut(block, upper, flat, at):
    half = block.shape[1] // 2
    for k in range(block.shape[0]):
        row = block[k].astype(jnp.float32)
        flat[pl.ds(at + k * half, half)] = jnp.where(upper, row[half:], row[:half])


def pack_kernel(mine, other, gain, weight, out, flat):
    upper = core_of() == 1
    cut(mine, upper, flat, 0)
    cut(other, upper, flat, flat.shape[0] // 2)
    out[...] = project(flat[...], gain[...], weight[...]).astype(out.dtype)


def split_kernel(block, kept, passed, flat):
    cut(block, core_of() == 1, flat, 0)
    kept[...] = flat[...].astype(kept.dtype)
    cut(block, core_of() == 0, flat, 0)
    passed[...] = flat[...].astype(passed.dtype)


def load_kernel(*refs):
    count = len(refs) // 2
    copies = [
        pltpu.make_async_copy(source, target, refs[-1].at[i])
        for i, (source, target) in enumerate(zip(refs[:count], refs[count:-1]))
    ]
    for copy in copies:
        copy.start()
    for copy in copies:
        copy.wait()


def gate_kernel(mine, gain, weight, out):
    rows, columns, width = mine.shape
    flat = mine[...].reshape(rows * columns, width).astype(jnp.float32)
    ready = norm_channels(flat, gain[...]).astype(jnp.bfloat16)
    out[...] = jax.nn.sigmoid(dot(ready, weight[...])).reshape(rows, columns, -1)


def add_block(left, right, sums, start=0, before=None):
    half, columns, width = sums.shape
    depth = left.shape[0] // half
    group = max(g for g in range(1, half + 1) if half % g == 0 and g * columns <= 288)
    for base in range(0, half, group):

        def step(k, totals):
            line = right[start + k]
            return tuple(
                total + left[pl.ds(k * half + base + i, 1)] * line
                for i, total in enumerate(totals)
            )

        totals = (jnp.zeros((columns, width), jnp.float32),) * group
        if before is not None:
            totals = tuple(before[base + i] for i in range(group))
        totals = lax.fori_loop(0, depth, step, totals, unroll=6)
        for i, total in enumerate(totals):
            sums[base + i] = total


def first_kernel(kept, mine, other, gain, right_weight, right, sums, left):
    rows, columns, width = mine.shape
    for part, block in enumerate((mine, other)):
        flat = project(block[...].reshape(rows * columns, width), gain[...], right_weight[...])
        right[pl.ds(part * rows, rows)] = flat.reshape(rows, columns, -1)
    left[...] = kept[...].astype(jnp.float32)
    add_block(left, right, sums)


def middle_kernel(*refs):
    right, left = refs[0], refs[-1]
    count = len(refs) // 2 - 1
    for block, sums in zip(refs[1 : 1 + count], refs[1 + count : -1]):
        left[...] = block[...].astype(jnp.float32)
        add_block(left, right, sums)


def share_kernel(block, right, gain, weight, sums, left):
    left[...] = project(block[...], gain[...], weight[...])
    add_block(left, right, sums)


def joined_kernel(block, right, gain, weight, before, sums, left):
    left[...] = project(block[...], gain[...], weight[...])
    add_block(left, right, sums, right.shape[0] // 2, before)


def last_kernel(step, steps, messages, merge, block, right, *refs):
    blocks, outs, (sums, left) = refs[: len(steps)], refs[len(steps) : -2], refs[-2:]
    first, second = lax.axis_index("first"), lax.axis_index("second")
    chip, core = first // 2, lax.rem(first, 2)
    for at, ready in zip(steps, blocks):
        sums[second ^ at] = ready[...]
    left[...] = block[...].astype(jnp.float32)
    add_block(left, right, sums.at[second ^ step])
    for out, (targets, cores) in zip(outs, messages):
        place = jnp.int32(0)
        for z, target in enumerate(targets):
            place = jnp.where(chip == z, target, place)
        place = place if merge == 1 else 2 * place + (core ^ cores)
        out[...] = sums[place].astype(out.dtype)


def final_kernel(merge, per, scale, *refs):
    parts, (gate, gain, weight, out) = refs[:-4], refs[-4:]
    core = core_of()
    half, columns, width = parts[0].shape
    for slot in range(merge):
        mine = parts[slot * per : (slot + 1) * per]
        total = sum(part[...].astype(jnp.float32) for part in mine)
        flat = total.reshape(half * columns, width) * scale
        scaled = norm_channels(flat, gain[...]).astype(jnp.bfloat16)
        result = dot(scaled, weight[...]).reshape(half, columns, -1)
        rows = pl.ds(0, half) if merge == 1 else pl.ds((core ^ slot) * half, half)
        out[rows] = (result * gate[rows]).astype(out.dtype)


def call(kernel, out_shapes, *operands, scratch=(), waits=(), space=pltpu.VMEM):
    many = isinstance(out_shapes, list)
    held = jax.tree.leaves(out_shapes) + list(operands) + list(scratch)
    held = sum(math.prod(ref.shape) * jnp.dtype(ref.dtype).itemsize for ref in held)
    return pl.pallas_call(
        kernel,
        out_shape=out_shapes,
        in_specs=[pl.BlockSpec(memory_space=space)] * len(operands),
        out_specs=[VMEM] * len(out_shapes) if many else VMEM,
        scratch_shapes=[*scratch, *waits],
        compiler_params=pltpu.CompilerParams(vmem_limit_bytes=held + (2 << 20)),
        cost_estimate=pl.CostEstimate(
            flops=1 << 24, bytes_accessed=100000, transcendentals=0
        ),
    )(*operands)


def shards(pair_rows, in_gain, left_weight, right_weight, mid_gain, out_weight, out_gate):
    firsts, seconds = lax.axis_size("first"), lax.axis_size("second")
    rows, columns, width = pair_rows.shape
    mix, wide = left_weight.shape[1], out_weight.shape[1]
    chips, half, depth = firsts // 2, columns // 2, 2 * rows
    merge = rows // half
    in_gain, mid_gain = in_gain.reshape(1, -1), mid_gain.reshape(1, -1)
    axes = ("first", "second")
    shape, f32 = jax.ShapeDtypeStruct, jnp.float32

    ring = [0, *range(1, chips, 2), *range(2, chips, 2)[::-1]]
    targets = [
        [ring[(ring.index(z) + step) % chips] for z in range(chips)] for step in range(chips)
    ]

    def swap(values, step=0, core=0, block=0):
        pairs = [
            (a * seconds + b, (2 * targets[step][a // 2] + (a % 2 ^ core)) * seconds + (b ^ block))
            for a in range(firsts)
            for b in range(seconds)
        ]
        return lax.ppermute(values, axes, pairs)

    lefts = [pltpu.VMEM((depth * half, mix), f32)]
    held = shape((half, columns, mix), f32)
    part = shape((rows * half, width), pair_rows.dtype)
    other = swap(pair_rows, core=1)
    early = swap(pair_rows, block=seconds - 1)
    arguments = (
        pair_rows,
        in_gain,
        right_weight,
        out_gate,
        left_weight,
        mid_gain,
        out_weight,
    )
    mine, in_gain, right_weight, out_gate, left_weight, mid_gain, out_weight = call(
        load_kernel,
        [shape(x.shape, x.dtype) for x in arguments],
        *[pltpu.with_memory_space_constraint(x, pltpu.HBM) for x in arguments],
        waits=[pltpu.SemaphoreType.DMA((len(arguments),))],
        space=pltpu.HBM,
    )
    kept = call(
        pack_kernel,
        shape((depth * half, mix), jnp.bfloat16),
        mine,
        other,
        in_gain,
        left_weight,
        scratch=[pltpu.VMEM((depth * half, width), f32)],
    )
    late = list(range(1, seconds - 1))
    blocks = [swap(kept, block=s) for s in late[:-1]]
    last = swap(kept, block=late[-1])
    right, own = call(
        first_kernel,
        [shape((depth, columns, mix), f32), held],
        kept,
        mine,
        other,
        in_gain,
        right_weight,
        scratch=lefts,
    )
    factors = (right, in_gain, left_weight)
    near, passed = call(split_kernel, [part, part], early, scratch=[pltpu.VMEM(part.shape, f32)])
    passed = swap(passed, core=1)
    parts = [pltpu.VMEM((rows * half, mix), f32)]
    share = call(share_kernel, held, near, *factors, scratch=parts)
    joined = call(joined_kernel, held, passed, *factors, share, scratch=parts)
    middle = call(middle_kernel, [held] * len(blocks), right, *blocks, scratch=lefts)
    cores = range(merge)
    messages = [(t, c) for t in [*range(1, chips), 0] for c in reversed(cores)]
    outgoing = call(
        functools.partial(
            last_kernel,
            late[-1],
            [0, seconds - 1, *late[:-1]],
            [(targets[t], c) for t, c in messages],
            merge,
        ),
        [shape((half, columns, mix), f32 if m == (0, 0) else jnp.bfloat16) for m in messages],
        last,
        right,
        own,
        joined,
        *middle,
        scratch=[pltpu.VMEM((seconds, half, columns, mix), f32), *lefts],
    )
    gate = call(gate_kernel, shape((rows, columns, wide), f32), mine, in_gain, out_gate)
    arrived = {
        (t, c): sent if (t, c) == (0, 0) else swap(sent, step=t, core=c)
        for (t, c), sent in zip(messages, outgoing)
    }
    parts = [arrived[t, c] for c in cores for t in range(chips)]
    return call(
        functools.partial(final_kernel, merge, chips, (rows * firsts) ** -0.5),
        shape((rows, columns, wide), jnp.bfloat16),
        *parts,
        gate,
        mid_gain,
        out_weight,
    )


def solution(mesh):
    in_specs = (P("first", "second", None), P(), P(), P(), P(), P(), P())
    out_specs = P("first", "second", None)
    return jax.shard_map(shards, mesh=mesh, in_specs=in_specs, out_specs=out_specs, check_vma=False)
```

```python
import functools
import math

import jax
import jax.numpy as jnp
from jax import lax
from jax.experimental import pallas as pl
from jax.experimental.pallas import tpu as pltpu
from jax.sharding import PartitionSpec as P


VMEM = pl.BlockSpec(memory_space=pltpu.VMEM)


def norm_channels(values, channel_gain):
    centred = values - jnp.mean(values, axis=-1, keepdims=True)
    variance = jnp.mean(centred * centred, axis=-1, keepdims=True)
    return centred * lax.rsqrt(variance + 1e-05) * channel_gain


def dot(rows, weight):
    return jnp.dot(rows, weight, preferred_element_type=jnp.float32)


def project(rows, gain, weight):
    ready = norm_channels(rows.astype(jnp.float32), gain).astype(jnp.bfloat16)
    return dot(ready, weight).astype(jnp.bfloat16).astype(jnp.float32)


def core_of():
    return lax.rem(lax.axis_index("first"), 2)


def cut(block, upper, flat, at):
    half = block.shape[1] // 2
    for k in range(block.shape[0]):
        row = block[k].astype(jnp.float32)
        flat[pl.ds(at + k * half, half)] = jnp.where(upper, row[half:], row[:half])


def pack_kernel(mine, other, gain, weight, out, flat):
    upper = core_of() == 1
    cut(mine, upper, flat, 0)
    cut(other, upper, flat, flat.shape[0] // 2)
    out[...] = project(flat[...], gain[...], weight[...]).astype(out.dtype)


def split_kernel(block, kept, passed, flat):
    cut(block, core_of() == 1, flat, 0)
    kept[...] = flat[...].astype(kept.dtype)
    cut(block, core_of() == 0, flat, 0)
    passed[...] = flat[...].astype(passed.dtype)


def load_kernel(*refs):
    count = len(refs) // 2
    copies = [
        pltpu.make_async_copy(source, target, refs[-1].at[i])
        for i, (source, target) in enumerate(zip(refs[:count], refs[count:-1]))
    ]
    for copy in copies:
        copy.start()
    for copy in copies:
        copy.wait()


def gate_kernel(mine, gain, weight, out):
    rows, columns, width = mine.shape
    flat = mine[...].reshape(rows * columns, width).astype(jnp.float32)
    ready = norm_channels(flat, gain[...]).astype(jnp.bfloat16)
    out[...] = jax.nn.sigmoid(dot(ready, weight[...])).reshape(rows, columns, -1)


def add_block(left, right, sums, start=0, before=None):
    half, columns, width = sums.shape
    depth = left.shape[0] // half
    group = max(g for g in range(1, half + 1) if half % g == 0 and g * columns <= 288)
    for base in range(0, half, group):

        def step(k, totals):
            line = right[start + k]
            return tuple(
                total + left[pl.ds(k * half + base + i, 1)] * line
                for i, total in enumerate(totals)
            )

        totals = (jnp.zeros((columns, width), jnp.float32),) * group
        if before is not None:
            totals = tuple(before[base + i] for i in range(group))
        totals = lax.fori_loop(0, depth, step, totals, unroll=12)
        for i, total in enumerate(totals):
            sums[base + i] = total


def first_kernel(kept, mine, other, gain, right_weight, right, sums, left):
    rows, columns, width = mine.shape
    for part, block in enumerate((mine, other)):
        flat = project(block[...].reshape(rows * columns, width), gain[...], right_weight[...])
        right[pl.ds(part * rows, rows)] = flat.reshape(rows, columns, -1)
    left[...] = kept[...].astype(jnp.float32)
    add_block(left, right, sums)


def middle_kernel(*refs):
    right, left = refs[0], refs[-1]
    count = len(refs) // 2 - 1
    for block, sums in zip(refs[1 : 1 + count], refs[1 + count : -1]):
        left[...] = block[...].astype(jnp.float32)
        add_block(left, right, sums)


def share_kernel(block, right, gain, weight, sums, left):
    left[...] = project(block[...], gain[...], weight[...])
    add_block(left, right, sums)


def joined_kernel(block, right, gain, weight, before, sums, left):
    left[...] = project(block[...], gain[...], weight[...])
    add_block(left, right, sums, right.shape[0] // 2, before)


def last_kernel(step, steps, messages, merge, block, right, *refs):
    blocks, outs, (sums, left) = refs[: len(steps)], refs[len(steps) : -2], refs[-2:]
    first, second = lax.axis_index("first"), lax.axis_index("second")
    chip, core = first // 2, lax.rem(first, 2)
    for at, ready in zip(steps, blocks):
        sums[second ^ at] = ready[...]
    left[...] = block[...].astype(jnp.float32)
    add_block(left, right, sums.at[second ^ step])
    for out, (targets, cores) in zip(outs, messages):
        place = jnp.int32(0)
        for z, target in enumerate(targets):
            place = jnp.where(chip == z, target, place)
        place = place if merge == 1 else 2 * place + (core ^ cores)
        out[...] = sums[place].astype(out.dtype)


def presum_kernel(*refs):
    refs[-1][...] = sum(part[...].astype(jnp.float32) for part in refs[:-1])


def final_kernel(merge, per, scale, *refs):
    parts, (gate, gain, weight, out) = refs[:-4], refs[-4:]
    core = core_of()
    half, columns, width = parts[0].shape
    for slot in range(merge):
        mine = parts[slot * per : (slot + 1) * per]
        total = sum(part[...].astype(jnp.float32) for part in mine)
        flat = total.reshape(half * columns, width) * scale
        scaled = norm_channels(flat, gain[...]).astype(jnp.bfloat16)
        result = dot(scaled, weight[...]).reshape(half, columns, -1)
        rows = pl.ds(0, half) if merge == 1 else pl.ds((core ^ slot) * half, half)
        out[rows] = (result * gate[rows]).astype(out.dtype)


def call(kernel, out_shapes, *operands, scratch=(), waits=(), space=pltpu.VMEM):
    many = isinstance(out_shapes, list)
    held = jax.tree.leaves(out_shapes) + list(operands) + list(scratch)
    held = sum(math.prod(ref.shape) * jnp.dtype(ref.dtype).itemsize for ref in held)
    return pl.pallas_call(
        kernel,
        out_shape=out_shapes,
        in_specs=[pl.BlockSpec(memory_space=space)] * len(operands),
        out_specs=[VMEM] * len(out_shapes) if many else VMEM,
        scratch_shapes=[*scratch, *waits],
        compiler_params=pltpu.CompilerParams(vmem_limit_bytes=held + (2 << 20)),
        cost_estimate=pl.CostEstimate(
            flops=1 << 24, bytes_accessed=100000, transcendentals=0
        ),
    )(*operands)


def shards(pair_rows, in_gain, left_weight, right_weight, mid_gain, out_weight, out_gate):
    firsts, seconds = lax.axis_size("first"), lax.axis_size("second")
    rows, columns, width = pair_rows.shape
    mix, wide = left_weight.shape[1], out_weight.shape[1]
    chips, half, depth = firsts // 2, columns // 2, 2 * rows
    merge = rows // half
    in_gain, mid_gain = in_gain.reshape(1, -1), mid_gain.reshape(1, -1)
    axes = ("first", "second")
    shape, f32 = jax.ShapeDtypeStruct, jnp.float32

    ring = [0, *range(1, chips, 2), *range(2, chips, 2)[::-1]]
    targets = [
        [ring[(ring.index(z) + step) % chips] for z in range(chips)] for step in range(chips)
    ]

    def swap(values, step=0, core=0, block=0):
        pairs = [
            (a * seconds + b, (2 * targets[step][a // 2] + (a % 2 ^ core)) * seconds + (b ^ block))
            for a in range(firsts)
            for b in range(seconds)
        ]
        return lax.ppermute(values, axes, pairs)

    lefts = [pltpu.VMEM((depth * half, mix), f32)]
    held = shape((half, columns, mix), f32)
    part = shape((rows * half, width), pair_rows.dtype)
    other = swap(pair_rows, core=1)
    early = swap(pair_rows, block=seconds - 1)
    arguments = (
        pair_rows,
        in_gain,
        right_weight,
        out_gate,
        left_weight,
        mid_gain,
        out_weight,
    )
    mine, in_gain, right_weight, out_gate, left_weight, mid_gain, out_weight = call(
        load_kernel,
        [shape(x.shape, x.dtype) for x in arguments],
        *[pltpu.with_memory_space_constraint(x, pltpu.HBM) for x in arguments],
        waits=[pltpu.SemaphoreType.DMA((len(arguments),))],
        space=pltpu.HBM,
    )
    kept = call(
        pack_kernel,
        shape((depth * half, mix), jnp.bfloat16),
        mine,
        other,
        in_gain,
        left_weight,
        scratch=[pltpu.VMEM((depth * half, width), f32)],
    )
    late = list(range(1, seconds - 1))
    blocks = [swap(kept, block=s) for s in late[:-1]]
    last = swap(kept, block=late[-1])
    right, own = call(
        first_kernel,
        [shape((depth, columns, mix), f32), held],
        kept,
        mine,
        other,
        in_gain,
        right_weight,
        scratch=lefts,
    )
    factors = (right, in_gain, left_weight)
    near, passed = call(split_kernel, [part, part], early, scratch=[pltpu.VMEM(part.shape, f32)])
    passed = swap(passed, core=1)
    parts = [pltpu.VMEM((rows * half, mix), f32)]
    share = call(share_kernel, held, near, *factors, scratch=parts)
    joined = call(joined_kernel, held, passed, *factors, share, scratch=parts)
    middle = call(middle_kernel, [held] * len(blocks), right, *blocks, scratch=lefts)
    cores = range(merge)
    messages = [(t, c) for t in [*range(1, chips), 0] for c in reversed(cores)]
    outgoing = call(
        functools.partial(
            last_kernel,
            late[-1],
            [0, seconds - 1, *late[:-1]],
            [(targets[t], c) for t, c in messages],
            merge,
        ),
        [shape((half, columns, mix), f32 if m == (0, 0) else jnp.bfloat16) for m in messages],
        last,
        right,
        own,
        joined,
        *middle,
        scratch=[pltpu.VMEM((seconds, half, columns, mix), f32), *lefts],
    )
    gate = call(gate_kernel, shape((rows, columns, wide), f32), mine, in_gain, out_gate)
    arrived = {
        (t, c): sent if (t, c) == (0, 0) else swap(sent, step=t, core=c)
        for (t, c), sent in zip(messages, outgoing)
    }
    parts = []
    for c in cores:
        *ready, latest = [arrived[t, c] for t in range(chips)]
        parts += [call(presum_kernel, held, *ready), latest]
    return call(
        functools.partial(final_kernel, merge, 2, (rows * firsts) ** -0.5),
        shape((rows, columns, wide), jnp.bfloat16),
        *parts,
        gate,
        mid_gain,
        out_weight,
    )


def solution(mesh):
    in_specs = (P("first", "second", None), P(), P(), P(), P(), P(), P())
    out_specs = P("first", "second", None)
    return jax.shard_map(shards, mesh=mesh, in_specs=in_specs, out_specs=out_specs, check_vma=False)
```
